256 devices in a mesh: seq: 32 (over z, x), head: 8 (over y, core).
Axes of the slice: x: 4, y: 4, z: 8, core: 2. Of those that a mesh axis runs over, the one named last changes fastest.
Arguments:
- queries: bfloat16 [16384, 4096], P('seq', 'head'), may hold values from -80 to 80
- new_keys: bfloat16 [16384, 1024], P('seq', 'head'), may hold values from -8 to 8
- new_values: bfloat16 [16384, 1024], P('seq', 'head'), may hold values from -6 to 6
Outputs:
- attended: bfloat16 [16384, 4096], P('seq', 'head')
- key_low: float32 [128, 1024], P('seq', 'head')
- key_step: float32 [128, 1024], P('seq', 'head')
- value_low: float32 [16384], P('seq')
- value_step: float32 [16384], P('seq')
The draws below stay inside these ranges and needn't reach their ends.
All inputs are finite; a program needn't handle non-finite values.
Results may differ from the reference program's by a relative error of at most 0.0045.
Values may be sent and summed in bfloat16 or wider, within the bound.
A program may use at most 64 MiB of HBM per device.

```python
import math
import jax
import jax.numpy as jnp
from jax import lax

HEADS = 32
KV_HEADS = 8
HEAD_DIM = 128
WINDOW = 4096
GROUP = 128
TOK_DEV = 512
TOKENS = 16384


def draw_pair(base):
    width = KV_HEADS * HEAD_DIM
    key_rows = jnp.clip(jax.random.normal(jax.random.fold_in(base, 1), (TOKENS, width), jnp.float32), -6.0, 6.0)
    query_rows = 2.0 * jnp.clip(jax.random.normal(jax.random.fold_in(base, 2), (TOKENS, HEADS * HEAD_DIM), jnp.float32), -6.0, 6.0)
    return (query_rows, key_rows)


def draw_queries(key, part):
    query_rows, key_rows = draw_pair(jax.random.fold_in(key, 7))
    return query_rows.astype(jnp.bfloat16)


def draw_new_keys(key, part):
    query_rows, key_rows = draw_pair(jax.random.fold_in(key, 7))
    return key_rows.astype(jnp.bfloat16)


def shard_levels(rng, shape, cuts, low, largest):
    def one(axis_at, blocks):
        draws = jax.random.uniform(jax.random.fold_in(jax.random.fold_in(rng, 6), axis_at), (blocks,), jnp.float32, low / len(cuts), largest / len(cuts))
        return jnp.repeat(jnp.exp(draws), shape[axis_at] // blocks).reshape((-1,) + (1,) * (len(shape) - axis_at - 1))

    factor_of = one(*cuts[0])
    for cut in cuts[1:]:
        factor_of = factor_of * one(*cut)
    return factor_of


def scatter_about(key, extent, scale, most, cuts=(), kind=jnp.bfloat16):
    array = jax.random.normal(key, extent, jnp.float32) * scale
    if len(cuts) > 0:
        array = shard_levels(key, extent, cuts, -0.22, 0.18) * array
    return jnp.clip(array, min=-most, max=most).astype(kind)


def setup_inputs(seed: int = 0) -> dict:
    streams_of = jax.random.split(jax.random.key(seed), 4)
    return {
        "queries": draw_queries(jax.random.fold_in(streams_of[3], 71), 0),
        "new_keys": draw_new_keys(jax.random.fold_in(streams_of[3], 71), 0),
        "new_values": scatter_about(streams_of[2], (TOKENS, KV_HEADS * HEAD_DIM), 1.0, 6.0, ((0, 32), (1, 8))),
    }


negative_fill = -1e+30

def attend_head(inputs, valid, scale):
    query_head, key_head, value_head = inputs
    scores = jnp.einsum('qgd,kd->gqk', query_head.astype(jnp.float32), key_head.astype(jnp.float32), precision=lax.Precision.HIGHEST) * scale
    masked = jnp.where(valid[None], scores, negative_fill)
    peak = lax.optimization_barrier(jnp.max(masked, axis=-1, keepdims=True))
    weights = jnp.where(valid[None], jnp.exp(masked - peak), 0.0)
    total = lax.optimization_barrier(jnp.sum(weights, axis=-1, keepdims=True))
    rounded = lax.optimization_barrier(weights.astype(jnp.bfloat16)).astype(jnp.float32)
    numer = jnp.einsum('gqk,kd->gqd', rounded, value_head.astype(jnp.float32), precision=lax.Precision.HIGHEST)
    return (numer / total).astype(jnp.bfloat16)

def reference(queries, new_keys, new_values):
    group_size = HEADS // KV_HEADS
    scale = 1.0 / math.sqrt(HEAD_DIM)
    block = TOK_DEV
    nblocks = TOKENS // block
    span = WINDOW + block
    zeros_front = jnp.zeros((WINDOW, KV_HEADS * HEAD_DIM), jnp.bfloat16)
    key_padded = jnp.concatenate((zeros_front, new_keys), 0)
    value_padded = jnp.concatenate((zeros_front, new_values), 0)

    def per_block(index):
        start = (index * block).astype(jnp.int32)
        query_block = lax.dynamic_slice_in_dim(queries, start, block, 0).reshape(block, KV_HEADS, group_size, HEAD_DIM)
        key_window = lax.dynamic_slice_in_dim(key_padded, start, span, 0).reshape(span, KV_HEADS, HEAD_DIM)
        value_window = lax.dynamic_slice_in_dim(value_padded, start, span, 0).reshape(span, KV_HEADS, HEAD_DIM)
        query_pos = start + jnp.arange(block, dtype=jnp.int32)
        key_pos = start - WINDOW + jnp.arange(span, dtype=jnp.int32)
        valid = (key_pos[None, :] <= query_pos[:, None]) & (key_pos[None, :] > query_pos[:, None] - WINDOW) & (key_pos[None, :] >= 0)
        heads_out = lax.map(lambda inputs: attend_head(inputs, valid, scale), (jnp.transpose(query_block, (1, 0, 2, 3)), jnp.transpose(key_window, (1, 0, 2)), jnp.transpose(value_window, (1, 0, 2))))
        return jnp.transpose(heads_out, (2, 0, 1, 3)).reshape(block, HEADS * HEAD_DIM)
    attended = lax.map(per_block, jnp.arange(nblocks, dtype=jnp.int32)).reshape(TOKENS, HEADS * HEAD_DIM)
    grouped = new_keys.astype(jnp.float32).reshape(TOKENS // GROUP, GROUP, KV_HEADS * HEAD_DIM)
    key_low = lax.optimization_barrier(jnp.min(grouped, axis=1))
    key_step = (lax.optimization_barrier(jnp.max(grouped, axis=1)) - key_low) / 3.0
    value_rows = new_values.astype(jnp.float32)
    value_low = lax.optimization_barrier(jnp.min(value_rows, axis=1))
    value_step = (lax.optimization_barrier(jnp.max(value_rows, axis=1)) - value_low) / 3.0
    return (attended, key_low, key_step, value_low, value_step)
```

```python
import functools
import math

import jax
import jax.numpy as jnp
from jax import lax
from jax.experimental import pallas as pl
from jax.experimental.pallas import tpu as pltpu
from jax.sharding import PartitionSpec as P

HEADS = 32
KV_HEADS = 8
HEAD_DIM = 128
WINDOW = 4096
GROUP = 128
PER = HEADS // KV_HEADS
TOK = 512
CHUNK = 128
TILE = 256
SPAN = TOK // TILE
XS = 4
ZS = 8
OWN = 32
LOG2E = 1.4426950408889634
SCALE = LOG2E / math.sqrt(HEAD_DIM)
NEG = -1e30

STARTS = (
    ((0, 34, 24), (1, 32, 2), (2, 33, 1), (0, 32, 2), (1, 34, 16), (2, 32, 0), (0, 33, 3), (1, 33, 3), (2, 34, 6)),
    ((0, 32, 0), (2, 33, 1), (0, 34, 14), (2, 32, 0), (0, 33, 1), (2, 34, 8)),
    ((0, 33, 1), (2, 34, 4), (0, 34, 18), (2, 33, 3), (0, 32, 0), (2, 32, 2)),
    ((2, 32, 6), (2, 34, 4), (2, 35, 5)),
)
STEPS = (
    (
        ((1, ((0, 1, 5), (1, 1, 9), (2, 1, 31))), (0, ((0, 0, 4), (1, 0, 8), (2, 0, 30)))),
        ((6, ((0, 6, 20), (1, 6, 20), (2, 6, 26), (2, 35, 7))), (18, ((0, 18, 18),)), (3, ((1, 3, 15), (1, 35, 17))), (31, ()), (4, ((0, 4, 14),)), (2, ((2, 2, 8),))),
        ((30, ()), (5, ((0, 5, 15),))),
        ((10, ((1, 10, 28), (2, 10, 20), (2, 4, 14))), (26, ()), (16, ((0, 16, 28),)), (9, ()), (7, ((1, 7, 21), (0, 7, 21), (2, 7, 27), (0, 35, 25)))),
        ((13, ()), (24, ()), (8, ())),
        ((12, ((2, 12, 22),)), (11, ((1, 11, 29),))),
        (),
        ((20, ()), (15, ()), (28, ()), (14, ())),
        ((17, ()),),
        ((23, ()), (27, ()), (19, ())),
        ((21, ()),),
        ((22, ()),),
        ((25, ()),),
        (),
        ((29, ()),),
        (),
    ),
    (
        ((24, ()), (1, ((1, 1, 3), (0, 1, 7), (2, 1, 31))), (2, ()), (0, ((1, 0, 2), (0, 0, 6), (2, 0, 30), (2, 35, 9)))),
        ((3, ((0, 3, 9),)),),
        ((8, ((1, 8, 10), (0, 8, 16), (2, 8, 26), (0, 35, 15))), (10, ()), (5, ()), (31, ((1, 31, 9), (1, 10, 24))), (7, ((2, 7, 13),)), (4, ())),
        ((30, ()), (6, ())),
        ((20, ((0, 20, 28),)), (9, ((1, 9, 11), (2, 9, 27), (0, 9, 17)))),
        ((16, ((1, 16, 28),)), (18, ()), (26, ()), (11, ((2, 11, 17),))),
        ((14, ((0, 14, 22), (2, 14, 22))), (13, ((1, 13, 23),)), (12, ())),
        ((15, ()),),
        ((27, ((1, 27, 21),)), (28, ()), (19, ((2, 19, 29),)), (17, ((1, 17, 29),))),
        (),
        ((21, ()),),
        ((23, ()), (22, ())),
        ((25, ()),),
        (),
        ((29, ()),),
        (),
    ),
    (
        ((0, ((0, 0, 12),)), (4, ((1, 4, 10), (2, 4, 26), (2, 35, 5))), (14, ()), (3, ((1, 3, 7), (0, 3, 11))), (1, ())),
        ((2, ((1, 2, 6), (0, 2, 10), (2, 2, 30), (0, 1, 13))),),
        ((8, ((2, 8, 10),)), (7, ()), (26, ((1, 26, 16),)), (12, ((2, 12, 20),)), (6, ()), (5, ((1, 5, 11), (0, 5, 23), (0, 35, 19), (2, 5, 27), (0, 14, 24), (2, 3, 31)))),
        (),
        ((18, ()), (9, ())),
        ((30, ((1, 30, 12),)), (11, ()), (16, ()), (10, ())),
        ((13, ((1, 13, 19), (2, 13, 21))),),
        ((15, ((0, 15, 25),)),),
        ((20, ()), (25, ((1, 25, 23),)), (28, ()), (27, ()), (23, ()), (17, ())),
        ((31, ()), (19, ())),
        ((22, ()), (21, ())),
        (),
        ((24, ()),),
        (),
        ((29, ()),),
        (),
    ),
    (
        ((1, ()), (2, ((1, 2, 8),)), (6, ((0, 6, 18), (2, 6, 30), (1, 6, 12), (2, 33, 7))), (18, ()), (16, ((1, 16, 18),)), (4, ((0, 4, 4),)), (0, ())),
        ((3, ()),),
        ((5, ((0, 5, 5), (2, 5, 27))),),
        ((12, ((2, 12, 14),)), (9, ((1, 9, 11),)), (30, ((0, 30, 16),)), (11, ((0, 11, 13),)), (8, ()), (7, ((1, 7, 13), (2, 7, 31), (2, 4, 26), (2, 18, 22)))),
        (),
        ((10, ((0, 10, 12),)),),
        ((20, ()), (27, ((1, 27, 25), (0, 27, 15), (1, 5, 23))), (13, ())),
        ((15, ()), (14, ())),
        ((23, ()), (17, ((1, 17, 19),))),
        ((31, ((0, 31, 17), (0, 7, 19), (0, 23, 25))), (19, ())),
        ((28, ()), (26, ((1, 26, 24),)), (24, ()), (21, ((1, 21, 29),))),
        ((22, ()),),
        ((25, ()),),
        (),
        ((29, ()),),
        (),
    ),
)
ROWS = ((1, 1, 0, 0), (1, 0, 1, 0), (1, 1, 1, 1), (1, 1, 1, 1), (2, 1, 0, 1), (1, 1, 1, 1), (1, 2, 1, 0), (2, 1, 0, 1), (2, 2, 1, 0), (1, 1, 0, 0), (2, 1, 2, 1), (2, 2, 1, 1), (1, 0, 2, 0), (2, 2, 2, 2), (2, 2, 1, 1), (2, 2, 2, 2))

MASKED_TAIL = 15
MASKED_HEAD = 13

STEP_SLOTS = tuple((2 * e, 2 * e + 1) for e in range(16))


def kernel(
    q_hbm, k_hbm, v_hbm,
    out_hbm, key_low, key_step, value_low, value_step,
    kv, qv, qt, acc, top, stat, gathered, out_v,
    local_sems, recv_sems, send_sems, stat_send, stat_recv, out_sems,
):
    seq = lax.axis_index("seq")
    head = lax.axis_index("head")
    x = lax.rem(seq, XS)
    z = lax.div(seq, XS)
    xp = z * XS + lax.rem(x + 1, XS)
    xm = z * XS + lax.rem(x + XS - 1, XS)
    zp = lax.rem(z + 1, ZS) * XS + x
    zm = lax.rem(z + ZS - 1, ZS) * XS + x
    link = (xp, xm, zp)

    load_k = pltpu.make_async_copy(k_hbm, kv.at[pl.ds(OWN, 4), 0], local_sems.at[0])
    load_v = pltpu.make_async_copy(v_hbm, kv.at[pl.ds(OWN, 4), 1], local_sems.at[1])
    load_q = pltpu.make_async_copy(q_hbm, qv, local_sems.at[2])
    load_k.start()
    load_v.start()
    load_q.start()

    barrier = pltpu.get_barrier_semaphore()
    for other in (xp, xm, zp, zm):
        pl.semaphore_signal(
            barrier, inc=1, device_id={"seq": other, "head": head}, device_id_type=pl.DeviceIdType.MESH
        )
    peers = [lax.rem(head + d, KV_HEADS) for d in range(1, KV_HEADS)]
    for peer in peers:
        pl.semaphore_signal(
            barrier, inc=1, device_id={"seq": seq, "head": peer}, device_id_type=pl.DeviceIdType.MESH
        )
    load_k.wait()
    load_v.wait()
    pl.semaphore_wait(barrier, 4 + KV_HEADS - 1)

    def send(d, src, dst):
        pltpu.make_async_remote_copy(
            src_ref=kv.at[src],
            dst_ref=kv.at[dst],
            send_sem=send_sems.at[d],
            recv_sem=recv_sems.at[dst],
            device_id={"seq": link[d], "head": head},
            device_id_type=pl.DeviceIdType.MESH,
        ).start()

    def arrived(slot):
        pltpu.make_async_copy(kv.at[slot], kv.at[slot], recv_sems.at[slot]).wait()

    for here in range(XS):
        @pl.when(x == here)
        def _():
            for d, src, dst in STARTS[here]:
                send(d, src, dst)

    own_v = [kv[OWN + c, 1].T for c in range(4)]
    for c in range(4):
        part = own_v[c].astype(jnp.float32)
        stat[0:1, pl.ds(c * CHUNK, CHUNK)] = jnp.max(part, axis=0, keepdims=True)
        stat[1:2, pl.ds(c * CHUNK, CHUNK)] = jnp.min(part, axis=0, keepdims=True)
        keys = kv[OWN + c, 0].astype(jnp.float32)
        low = jnp.min(keys, axis=0, keepdims=True)
        key_low[pl.ds(c, 1), :] = low
        key_step[pl.ds(c, 1), :] = (jnp.max(keys, axis=0, keepdims=True) - low) / 3.0

    load_q.wait()
    for t in range(SPAN * PER):
        p, h = divmod(t, PER)
        part = qv[pl.ds(p * TILE, TILE), pl.ds(h * HEAD_DIM, HEAD_DIM)].T.astype(jnp.float32) * SCALE
        high = part.astype(jnp.bfloat16)
        qt[t, 0:HEAD_DIM, :] = high
        qt[t, HEAD_DIM:, :] = (part - high.astype(jnp.float32)).astype(jnp.bfloat16)

    ones = jnp.ones((16, 2 * CHUNK), jnp.bfloat16)

    def attend(slots, modes, first=False):
        keys = jnp.concatenate([kv[slots[0], 0], kv[slots[1], 0]], axis=0)
        keys = jnp.concatenate([keys, keys], axis=1)
        values = jnp.concatenate([kv[slots[0], 1].T, kv[slots[1], 1].T], axis=1)
        values = jnp.concatenate([values, ones], axis=0)
        for t in range(SPAN * PER):
            mode = modes[t // PER]
            if mode is None:
                continue
            s = jnp.dot(keys, qt[t], preferred_element_type=jnp.float32)
            if mode != "all":
                row = lax.broadcasted_iota(jnp.int32, s.shape, 0)
                col = lax.broadcasted_iota(jnp.int32, s.shape, 1)
                s = jnp.where(row <= col if mode == "past" else row > col, s, NEG)
            peak = jnp.max(s, axis=0, keepdims=True)
            if first:
                w = jnp.exp2(s - peak).astype(jnp.bfloat16)
                acc[t] = jnp.dot(values, w, preferred_element_type=jnp.float32)
                top[t] = peak
            else:
                old = top[t]
                new = jnp.maximum(old, peak)
                w = jnp.exp2(s - new).astype(jnp.bfloat16)
                part = jnp.dot(values, w, preferred_element_type=jnp.float32)
                acc[t] = acc[t] * jnp.exp2(old - new) + part
                top[t] = new

    attend((OWN, OWN + 1), ("past", "all"), first=True)

    for d, peer in enumerate(peers):
        pltpu.make_async_remote_copy(
            src_ref=stat,
            dst_ref=gathered.at[head],
            send_sem=stat_send.at[d],
            recv_sem=stat_recv.at[head],
            device_id={"seq": seq, "head": peer},
            device_id_type=pl.DeviceIdType.MESH,
        ).start()

    attend((OWN + 2, OWN + 3), (None, "past"))

    for e in range(16):
        for here in range(XS):
            @pl.when(x == here)
            def _():
                for slot, sends in STEPS[here][e]:
                    arrived(slot)
                    for d, src, dst in sends:
                        send(d, src, dst)
        rows = ROWS[e]
        modes = ("all", "all")
        if e == MASKED_HEAD:
            modes = ("all", "after")
        if e == MASKED_TAIL:
            modes = ("after", None)
        need = jnp.int32(rows[0])
        for here in range(1, XS):
            need = jnp.where(x == here, rows[here], need)

        @pl.when(z >= need)
        def _():
            attend(STEP_SLOTS[e], modes)

        if e == 5:
            most, least = stat[0:1, :], stat[1:2, :]
            for d in range(1, KV_HEADS):
                peer = peers[d - 1]
                pltpu.make_async_copy(gathered.at[peer], gathered.at[peer], stat_recv.at[peer]).wait()
                most = jnp.maximum(most, gathered[peer, 0:1, :])
                least = jnp.minimum(least, gathered[peer, 1:2, :])
            value_low[...] = least
            value_step[...] = (most - least) / 3.0

    copies = []
    for t in range(SPAN * PER):
        p, h = divmod(t, PER)
        full = acc[t]
        part = (full[0:HEAD_DIM] / full[HEAD_DIM : HEAD_DIM + 1]).astype(jnp.bfloat16)
        out_v[pl.ds(p * TILE, TILE), pl.ds(h * HEAD_DIM, HEAD_DIM)] = part.T
        if h == PER - 1:
            rows = pl.ds(p * TILE, TILE)
            copies.append(pltpu.make_async_copy(out_v.at[rows], out_hbm.at[rows], out_sems.at[p]))
            copies[-1].start()

    for d in range(KV_HEADS - 1):
        pltpu.make_async_copy(stat, stat, stat_send.at[d]).wait()
    for here in range(XS):
        @pl.when(x == here)
        def _():
            for d in range(3):
                count = sum(1 for s in STARTS[here] if s[0] == d)
                count += sum(1 for step in STEPS[here] for _, sends in step for s in sends if s[0] == d)
                block = kv.at[pl.ds(0, count)]
                pltpu.make_async_copy(block, block, send_sems.at[d]).wait()
    for copy in copies:
        copy.wait()


def shards(queries, new_keys, new_values):
    hbm = pl.BlockSpec(memory_space=pl.ANY)
    vmem = pl.BlockSpec(memory_space=pltpu.VMEM)
    f32, bf16 = jnp.float32, jnp.bfloat16
    tiles = SPAN * PER
    attended, key_low, key_step, value_low, value_step = pl.pallas_call(
        kernel,
        out_shape=(
            jax.ShapeDtypeStruct((TOK, PER * HEAD_DIM), bf16),
            jax.ShapeDtypeStruct((TOK // GROUP, HEAD_DIM), f32),
            jax.ShapeDtypeStruct((TOK // GROUP, HEAD_DIM), f32),
            jax.ShapeDtypeStruct((1, TOK), f32),
            jax.ShapeDtypeStruct((1, TOK), f32),
        ),
        in_specs=[hbm, hbm, hbm],
        out_specs=(hbm, vmem, vmem, vmem, vmem),
        scratch_shapes=[
            pltpu.VMEM((OWN + 4, 2, CHUNK, HEAD_DIM), bf16),
            pltpu.VMEM((TOK, PER * HEAD_DIM), bf16),
            pltpu.VMEM((tiles, 2 * HEAD_DIM, TILE), bf16),
            pltpu.VMEM((tiles, HEAD_DIM + 16, TILE), f32),
            pltpu.VMEM((tiles, 1, TILE), f32),
            pltpu.VMEM((2, TOK), f32),
            pltpu.VMEM((KV_HEADS, 2, TOK), f32),
            pltpu.VMEM((TOK, PER * HEAD_DIM), bf16),
            pltpu.SemaphoreType.DMA((3,)),
            pltpu.SemaphoreType.DMA((OWN,)),
            pltpu.SemaphoreType.DMA((3,)),
            pltpu.SemaphoreType.DMA((KV_HEADS - 1,)),
            pltpu.SemaphoreType.DMA((KV_HEADS,)),
            pltpu.SemaphoreType.DMA((SPAN,)),
        ],
        compiler_params=pltpu.CompilerParams(collective_id=0, has_side_effects=True),
    )(
        queries,
        new_keys.reshape(TOK // CHUNK, CHUNK, HEAD_DIM),
        new_values.reshape(TOK // CHUNK, CHUNK, HEAD_DIM),
    )
    return attended, key_low, key_step, value_low.reshape(TOK), value_step.reshape(TOK)


def solution(mesh):
    return jax.shard_map(
        shards,
        mesh=mesh,
        in_specs=(P("seq", "head"), P("seq", "head"), P("seq", "head")),
        out_specs=(P("seq", "head"), P("seq", "head"), P("seq", "head"), P("seq"), P("seq")),
        check_vma=False,
    )
```

```python
import math

import jax
import jax.numpy as jnp
from jax import lax
from jax.experimental import pallas as pl
from jax.experimental.pallas import tpu as pltpu
from jax.sharding import PartitionSpec as P

HEADS = 32
KV_HEADS = 8
HEAD_DIM = 128
WINDOW = 4096
GROUP = 128
PER = HEADS // KV_HEADS
TOK = 512
CHUNK = 128
TILE = 256
TILES = TOK // TILE * PER
DEEP = HEAD_DIM + 16
XS = 4
ZS = 8
OWN = 32
STEPS = 16
SCALE = 1.4426950408889634 / math.sqrt(HEAD_DIM)
NEG = -1e30
MESH = pl.DeviceIdType.MESH

PLAN = (
    (
        (2056, 6146, 10240, 2241, 6211, 10305, 2176, 6296, 10372, 12288, 4, 4104, 8222, 10437, 12352, 69, 4169, 8287, 12544, 270, 4372, 2121, 8476, 12480, 13504, 5327, 14208, 12416, 12672, 4496, 12608, 335, 8541, 12800, 12736, 4561, 8651, 4437, 6361, 14272, 12864, 595, 13056, 8982, 8785, 14080, 13184, 916, 13824, 14144, 13312, 1050, 12928, 12992, 13120, 9047, 14016, 13696, 13248, 13568, 13376, 13440, 13632, 13760, 13888, 13952),
        (9, 18, 28, 33, 39, 42, 54, 56, 59, 61, 62, 63, 64, 65, 66, 66, 66),
        (1, 1, 1, 1, 1, 2, 1, 2, 2, 1, 2, 2, 1, 2, 2, 2),
        (11, 11, 12),
    ),
    (
        (2121, 10443, 2241, 10242, 2176, 10307, 12800, 526, 12992, 4819, 8925, 12352, 12416, 4230, 140, 8350, 12288, 16, 2056, 12480, 4295, 8415, 10378, 205, 13824, 5644, 12544, 14144, 12672, 4504, 8592, 12608, 14208, 6026, 5979, 12736, 8657, 13184, 918, 81, 14272, 13120, 12864, 12928, 8860, 9750, 13056, 13248, 983, 13312, 5140, 13440, 13376, 5205, 13504, 1243, 9435, 13632, 14080, 5914, 13568, 13760, 13696, 13952, 13888, 14016),
        (6, 19, 24, 32, 37, 43, 46, 47, 49, 54, 57, 61, 63, 65, 66, 66, 66),
        (0, 1, 1, 1, 0, 1, 1, 1, 2, 1, 2, 2, 1, 2, 2, 2),
        (12, 10, 12),
    ),
    (
        (2048, 10372, 2113, 10242, 2253, 10307, 10437, 12864, 603, 12544, 4376, 12352, 12416, 4230, 138, 8350, 83, 12288, 8212, 12480, 4295, 12736, 4557, 8659, 13184, 12608, 343, 2188, 8541, 8476, 8415, 8277, 12672, 4492, 13056, 14208, 13952, 5778, 13312, 13568, 1294, 18, 12928, 12800, 538, 13504, 5333, 12992, 13120, 14144, 5975, 4441, 13824, 13696, 14080, 13248, 13376, 14272, 13440, 13760, 13632, 13888, 14016),
        (7, 19, 21, 32, 34, 45, 48, 49, 56, 57, 59, 61, 61, 62, 63, 63, 63),
        (0, 1, 1, 1, 0, 1, 1, 0, 0, 2, 1, 1, 2, 1, 2, 2),
        (11, 9, 11),
    ),
    (
        (10309, 10244, 10374, 10439, 12288, 12416, 12608, 323, 4423, 12352, 12480, 12544, 258, 4358, 8478, 13120, 13824, 12672, 392, 4506, 8604, 8267, 8543, 14016, 12800, 4618, 12736, 457, 8669, 12928, 12864, 4683, 14208, 1934, 13504, 13568, 14080, 1808, 5912, 4303, 6034, 13760, 1485, 13248, 12992, 13056, 8982, 13312, 14272, 1999, 13184, 914, 729, 13376, 14144, 5977, 13440, 13632, 13696, 13952, 13888),
        (4, 10, 11, 15, 29, 32, 45, 47, 53, 54, 57, 58, 59, 61, 61, 61, 61),
        (0, 0, 1, 1, 1, 1, 0, 1, 1, 0, 1, 1, 0, 0, 2, 2),
        (10, 9, 10),
    ),
)
OPS = max(len(plan[0]) for plan in PLAN)


def kernel(
    q_hbm, k_hbm, v_hbm,
    acc, key_stats, value_stats,
    kv, qv, qt, scores, weights, factor, top, held, stat, gathered, ops, bounds, rows,
    local_sems, recv_sems, send_sems, stat_send, stat_recv,
):
    seq = lax.axis_index("seq")
    head = lax.axis_index("head")
    x = lax.rem(seq, XS)
    z = lax.div(seq, XS)
    xp = z * XS + lax.rem(x + 1, XS)
    xm = z * XS + lax.rem(x + XS - 1, XS)
    zp = lax.rem(z + 1, ZS) * XS + x
    zm = lax.rem(z + ZS - 1, ZS) * XS + x
    peers = [lax.rem(head + d, KV_HEADS) for d in range(1, KV_HEADS)]

    load_k = pltpu.make_async_copy(k_hbm, kv.at[pl.ds(OWN, 4), 0], local_sems.at[0])
    load_v = pltpu.make_async_copy(v_hbm, kv.at[pl.ds(OWN, 4), 1], local_sems.at[1])
    load_q = pltpu.make_async_copy(q_hbm, qv, local_sems.at[2])
    load_k.start()
    load_v.start()
    load_q.start()

    barrier = pltpu.get_barrier_semaphore()
    for other in (xp, xm, zp, zm):
        pl.semaphore_signal(barrier, inc=1, device_id={"seq": other, "head": head}, device_id_type=MESH)
    for peer in peers:
        pl.semaphore_signal(barrier, inc=1, device_id={"seq": seq, "head": peer}, device_id_type=MESH)

    for here in range(XS):
        @pl.when(x == here)
        def _():
            plan_ops, plan_bounds, plan_rows, _ = PLAN[here]
            for i, value in enumerate(plan_ops):
                ops[i] = value
            for i, value in enumerate(plan_bounds):
                bounds[i] = value
            for i, value in enumerate(plan_rows):
                rows[i] = value

    load_k.wait()
    load_v.wait()
    pl.semaphore_wait(barrier, 4 + KV_HEADS - 1)

    def operate(i, carry):
        value = ops[i]
        kind = lax.div(value, 4096)
        src = lax.rem(lax.div(value, 64), 64)
        dst = lax.rem(value, 64)

        @pl.when(kind == 3)
        def _():
            pltpu.make_async_copy(kv.at[src], kv.at[src], recv_sems.at[src]).wait()

        @pl.when(kind < 3)
        def _():
            there = jnp.where(kind == 0, xp, jnp.where(kind == 1, xm, zp))
            pltpu.make_async_remote_copy(
                src_ref=kv.at[src],
                dst_ref=kv.at[dst],
                send_sem=send_sems.at[kind],
                recv_sem=recv_sems.at[dst],
                device_id={"seq": there, "head": head},
                device_id_type=MESH,
            ).start()

        return carry

    lax.fori_loop(0, bounds[0], operate, 0)

    for c in range(4):
        part = kv[OWN + c, 1].T.astype(jnp.float32)
        stat[0:1, pl.ds(c * CHUNK, CHUNK)] = jnp.max(part, axis=0, keepdims=True)
        stat[1:2, pl.ds(c * CHUNK, CHUNK)] = jnp.min(part, axis=0, keepdims=True)
        keys = kv[OWN + c, 0].astype(jnp.float32)
        low = jnp.min(keys, axis=0, keepdims=True)
        key_stats[pl.ds(c, 1), :] = low
        key_stats[pl.ds(4 + c, 1), :] = (jnp.max(keys, axis=0, keepdims=True) - low) / 3.0

    load_q.wait()
    for t in range(TILES):
        p, h = divmod(t, PER)
        part = qv[pl.ds(p * TILE, TILE), pl.ds(h * HEAD_DIM, HEAD_DIM)].T.astype(jnp.float32) * SCALE
        high = part.astype(jnp.bfloat16)
        qt[t, 0:HEAD_DIM, :] = high
        qt[t, HEAD_DIM:, :] = (part - high.astype(jnp.float32)).astype(jnp.bfloat16)
        top[t] = jnp.full((1, TILE), NEG, jnp.float32)
        acc[t] = jnp.zeros((DEEP, TILE), jnp.float32)

    def score(keys, t, mode):
        s = jnp.dot(keys, qt[t], preferred_element_type=jnp.float32)
        if mode != "all":
            row = lax.broadcasted_iota(jnp.int32, s.shape, 0)
            col = lax.broadcasted_iota(jnp.int32, s.shape, 1)
            s = jnp.where(row <= col if mode == "past" else row > col, s, NEG)
        scores[t] = s

    def weigh(t):
        s = scores[t]
        old = top[t]
        new = jnp.maximum(old, jnp.max(s, axis=0, keepdims=True))
        weights[t] = jnp.exp2(s - new).astype(jnp.bfloat16)
        factor[t] = jnp.exp2(old - new)
        top[t] = new

    def gather(values, t):
        acc[t] = acc[t] * factor[t] + jnp.dot(values, weights[t], preferred_element_type=jnp.float32)

    def attend(first, second, modes, before=True, after=True):
        past = held[...]
        keys = jnp.concatenate([kv[first, 0], kv[second, 0]], axis=0)
        keys = jnp.concatenate([keys, keys], axis=1)
        values = jnp.concatenate([kv[first, 1].T, kv[second, 1].T], axis=1)
        values = jnp.concatenate([values, jnp.ones((DEEP - HEAD_DIM, 2 * CHUNK), jnp.bfloat16)], axis=0)
        jobs = [t for t in range(TILES) if modes[t // PER] is not None]
        to_weigh = ([6, 7] if before else [None, None]) + jobs
        to_gather = ([4, 5, 6, 7] if before else [None] * 4) + jobs
        for i, t in enumerate(jobs):
            score(keys, t, modes[t // PER])
            if to_weigh[i] is not None:
                weigh(to_weigh[i])
            if to_gather[i] is not None:
                gather(past if i < 4 else values, to_gather[i])
        if after:
            held[...] = values
        else:
            for t in to_weigh[len(jobs):]:
                weigh(t)
            for t in to_gather[len(jobs):]:
                gather(values, t)

    attend(OWN, OWN + 1, ("past", "all"), before=False)

    for d, peer in enumerate(peers):
        pltpu.make_async_remote_copy(
            src_ref=stat,
            dst_ref=gathered.at[head],
            send_sem=stat_send.at[d],
            recv_sem=stat_recv.at[head],
            device_id={"seq": seq, "head": peer},
            device_id_type=MESH,
        ).start()

    attend(OWN + 2, OWN + 3, (None, "past"))

    def step(e, carry):
        lax.fori_loop(bounds[e], bounds[e + 1], operate, 0)

        @pl.when(z >= rows[e])
        def _():
            attend(2 * e, 2 * e + 1, ("all", "all"))

        return carry

    lax.fori_loop(0, STEPS - 2, step, 0)

    most, least = stat[0:1, :], stat[1:2, :]
    for peer in peers:
        pltpu.make_async_copy(gathered.at[peer], gathered.at[peer], stat_recv.at[peer]).wait()
        most = jnp.maximum(most, gathered[peer, 0:1, :])
        least = jnp.minimum(least, gathered[peer, 1:2, :])
    value_stats[0:1, :] = least
    value_stats[1:2, :] = (most - least) / 3.0

    lax.fori_loop(bounds[STEPS - 2], bounds[STEPS], operate, 0)

    @pl.when(z >= 2)
    def _():
        attend(2 * STEPS - 4, 2 * STEPS - 3, ("all", "after"))
        attend(2 * STEPS - 2, 2 * STEPS - 1, ("after", None), after=False)

    @pl.when(z < 2)
    def _():
        past = held[...]
        for t in (6, 7):
            weigh(t)
        for t in (4, 5, 6, 7):
            gather(past, t)

    for d in range(KV_HEADS - 1):
        pltpu.make_async_copy(stat, stat, stat_send.at[d]).wait()
    for here in range(XS):
        @pl.when(x == here)
        def _():
            for d, count in enumerate(PLAN[here][3]):
                block = kv.at[pl.ds(0, count)]
                pltpu.make_async_copy(block, block, send_sems.at[d]).wait()


def finish(acc, key_stats, value_stats, out_hbm, key_low, key_step, value_low, value_step, out_v, sems):
    copies = []
    for t in range(TILES):
        p, h = divmod(t, PER)
        part = acc[t, 0:HEAD_DIM] / acc[t, HEAD_DIM : HEAD_DIM + 1]
        out_v[pl.ds(p * TILE, TILE), pl.ds(h * HEAD_DIM, HEAD_DIM)] = part.astype(jnp.bfloat16).T
        if h == PER - 1:
            block = pl.ds(p * TILE, TILE)
            copies.append(pltpu.make_async_copy(out_v.at[block], out_hbm.at[block], sems.at[p]))
            copies[-1].start()
    key_low[...] = key_stats[0:4, :]
    key_step[...] = key_stats[4:8, :]
    value_low[...] = value_stats[0:1, :]
    value_step[...] = value_stats[1:2, :]
    for copy in copies:
        copy.wait()


def shards(queries, new_keys, new_values):
    hbm = pl.BlockSpec(memory_space=pl.ANY)
    vmem = pl.BlockSpec(memory_space=pltpu.VMEM)
    f32, bf16 = jnp.float32, jnp.bfloat16
    chunks = TOK // CHUNK
    state = pl.pallas_call(
        kernel,
        out_shape=(
            pltpu.VMEM((TILES, DEEP, TILE), f32),
            pltpu.VMEM((2 * chunks, HEAD_DIM), f32),
            pltpu.VMEM((2, TOK), f32),
        ),
        in_specs=[hbm, hbm, hbm],
        out_specs=(vmem, vmem, vmem),
        scratch_shapes=[
            pltpu.VMEM((OWN + 4, 2, CHUNK, HEAD_DIM), bf16),
            pltpu.VMEM((TOK, PER * HEAD_DIM), bf16),
            pltpu.VMEM((TILES, 2 * HEAD_DIM, TILE), bf16),
            pltpu.VMEM((TILES, 2 * CHUNK, TILE), f32),
            pltpu.VMEM((TILES, 2 * CHUNK, TILE), bf16),
            pltpu.VMEM((TILES, 1, TILE), f32),
            pltpu.VMEM((TILES, 1, TILE), f32),
            pltpu.VMEM((DEEP, 2 * CHUNK), bf16),
            pltpu.VMEM((2, TOK), f32),
            pltpu.VMEM((KV_HEADS, 2, TOK), f32),
            pltpu.SMEM((OPS,), jnp.int32),
            pltpu.SMEM((STEPS + 1,), jnp.int32),
            pltpu.SMEM((STEPS,), jnp.int32),
            pltpu.SemaphoreType.DMA((3,)),
            pltpu.SemaphoreType.DMA((OWN,)),
            pltpu.SemaphoreType.DMA((3,)),
            pltpu.SemaphoreType.DMA((KV_HEADS - 1,)),
            pltpu.SemaphoreType.DMA((KV_HEADS,)),
        ],
        compiler_params=pltpu.CompilerParams(collective_id=0, has_side_effects=True),
    )(
        queries,
        new_keys.reshape(chunks, CHUNK, HEAD_DIM),
        new_values.reshape(chunks, CHUNK, HEAD_DIM),
    )
    state = [pltpu.with_memory_space_constraint(part, pltpu.VMEM) for part in state]
    attended, key_low, key_step, value_low, value_step = pl.pallas_call(
        finish,
        out_shape=(
            jax.ShapeDtypeStruct((TOK, PER * HEAD_DIM), bf16),
            jax.ShapeDtypeStruct((TOK // GROUP, HEAD_DIM), f32),
            jax.ShapeDtypeStruct((TOK // GROUP, HEAD_DIM), f32),
            jax.ShapeDtypeStruct((1, TOK), f32),
            jax.ShapeDtypeStruct((1, TOK), f32),
        ),
        in_specs=[vmem, vmem, vmem],
        out_specs=(hbm, vmem, vmem, vmem, vmem),
        scratch_shapes=[
            pltpu.VMEM((TOK, PER * HEAD_DIM), bf16),
            pltpu.SemaphoreType.DMA((TOK // TILE,)),
        ],
    )(*state)
    return attended, key_low, key_step, value_low.reshape(TOK), value_step.reshape(TOK)


def solution(mesh):
    return jax.shard_map(
        shards,
        mesh=mesh,
        in_specs=(P("seq", "head"), P("seq", "head"), P("seq", "head")),
        out_specs=(P("seq", "head"), P("seq", "head"), P("seq", "head"), P("seq"), P("seq")),
        check_vma=False,
    )
```

```python
import math

import jax
import jax.numpy as jnp
from jax import lax
from jax.experimental import pallas as pl
from jax.experimental.pallas import tpu as pltpu
from jax.sharding import PartitionSpec as P

HEADS = 32
KV_HEADS = 8
HEAD_DIM = 128
WINDOW = 4096
GROUP = 128
PER = HEADS // KV_HEADS
TOK = 512
CHUNK = 128
TILE = 256
TILES = TOK // TILE * PER
DEEP = HEAD_DIM + 16
XS = 4
ZS = 8
REACH = 3
OWN = 32
STEPS = 15
SCALE = 1.4426950408889634 / math.sqrt(HEAD_DIM)
NEG = -1e30
MESH = pl.DeviceIdType.MESH

PLAN = (
    (
        (34881, 18434, 2255, 34816, 2121, 18631, 18499, 35011, 53312, 34946, 18566, 4163, 20557, 36941, 53248, 4098, 20492, 36876, 53440, 4299, 20689, 37071, 53632, 53568, 4437, 53376, 4234, 20624, 37006, 54272, 53504, 2190, 4372, 58176, 53696, 20957, 37331, 53824, 58112, 58496, 53760, 4632, 37404, 58304, 53952, 21211, 37595, 53888, 37530, 58240, 54336, 58816, 58560, 54528, 38174, 54592, 59136, 10014, 58880, 58752, 59072, 58944, 59008, 59200, 59328, 59264),
        (8, 18, 29, 33, 37, 43, 49, 50, 53, 55, 58, 60, 62, 63, 64, 66),
        (1, 1, 1, 1, 1, 1, 2, 1, 2, 1, 2, 2, 2, 2, 2),
        ((3, 7, 1), (4, 6, 0), (4, 9, 0)),
        6,
    ),
    (
        (2241, 2176, 34944, 34820, 2117, 2052, 35009, 50112, 991, 53248, 4104, 20486, 36882, 49728, 34885, 53504, 4368, 20752, 37136, 53312, 20551, 36947, 53440, 53696, 58496, 25746, 53376, 4238, 54080, 21323, 37723, 53568, 4433, 20817, 37201, 53952, 53632, 20884, 37270, 58368, 25624, 54592, 5461, 38237, 49664, 58560, 53888, 54016, 59072, 9945, 50048, 926, 54848, 38495, 58432, 25689, 54528, 58816, 26079, 58752, 54784, 59008, 59200, 59136, 59328, 59264),
        (7, 22, 28, 35, 39, 45, 47, 48, 52, 56, 57, 60, 61, 63, 64, 66),
        (1, 1, 1, 1, 0, 1, 1, 0, 2, 1, 2, 1, 2, 2, 2),
        ((6, 5, 1), (0, 6, 4), (4, 8, 0)),
        8,
    ),
    (
        (35011, 34887, 34946, 2068, 2249, 49216, 34822, 75, 32841, 53440, 2184, 20679, 37083, 49152, 10, 53696, 20941, 49472, 339, 53376, 4238, 20614, 37018, 49792, 17032, 49408, 274, 53632, 20876, 37272, 54528, 2133, 38162, 51136, 34775, 53824, 54080, 21337, 37725, 53760, 59072, 26327, 49856, 54272, 5150, 59008, 54016, 37660, 54144, 58880, 26138, 54208, 58496, 25756, 54336, 58560, 54720, 54592, 54656, 59200, 58944, 59136, 51072),
        (5, 15, 23, 27, 30, 40, 43, 48, 52, 55, 56, 58, 59, 61, 63, 63),
        (0, 1, 0, 1, 1, 0, 1, 1, 1, 2, 1, 1, 2, 2, 0),
        ((8, 2, 0), (1, 5, 3), (6, 6, 0)),
        12,
    ),
    (
        (34881, 34816, 35013, 50432, 34948, 34074, 53312, 4165, 36951, 49280, 16522, 49728, 33359, 53248, 4100, 20500, 36886, 49600, 53568, 4425, 20813, 37209, 49344, 16587, 49856, 53504, 4360, 20748, 37144, 49536, 49664, 54912, 5770, 54080, 21327, 49792, 33436, 58816, 9687, 26067, 54016, 50368, 34015, 54208, 5077, 54336, 54144, 58752, 9622, 54272, 21526, 50304, 58944, 9821, 55104, 50496, 58880, 54976, 55168, 55040, 55232),
        (3, 17, 24, 29, 31, 33, 37, 41, 47, 51, 52, 56, 57, 59, 60, 61),
        (1, 0, 1, 0, 0, 0, 1, 1, 1, 0, 0, 2, 1, 1, 1),
        ((0, 6, 3), (2, 5, 1), (8, 4, 0)),
        11,
    ),
)
OPS = max(len(plan[0]) for plan in PLAN)
TAIL_OUT = ((2, 3), (0, 1, 2, 3))
FULL_OUT = ((6, 7), (4, 5, 6, 7))


def kernel(
    q_hbm, k_hbm, v_hbm,
    acc, key_low, key_step, value_low, value_step,
    kv, qv, qt, scores, weights, factor, top, held, stat, gathered, ops, bounds, rows,
    local_sems, recv_sems, send_sems, stat_send, stat_recv,
):
    seq = lax.axis_index("seq")
    head = lax.axis_index("head")
    x = lax.rem(seq, XS)
    z = lax.div(seq, XS)
    xp = z * XS + lax.rem(x + 1, XS)
    xm = z * XS + lax.rem(x + XS - 1, XS)
    first_row, last_row = z == 0, z == ZS - 1
    zp = jnp.where(last_row, seq, seq + XS)
    zm = jnp.where(first_row, seq, seq - XS)
    peers = [lax.rem(head + d, KV_HEADS) for d in range(1, KV_HEADS)]

    load_k = pltpu.make_async_copy(k_hbm, kv.at[pl.ds(OWN, 4), 0], local_sems.at[0])
    load_v = pltpu.make_async_copy(v_hbm, kv.at[pl.ds(OWN, 4), 1], local_sems.at[1])
    load_q = pltpu.make_async_copy(q_hbm, qv, local_sems.at[2])
    load_k.start()
    load_v.start()
    load_q.start()

    barrier = pltpu.get_barrier_semaphore()

    def greet(other):
        pl.semaphore_signal(barrier, inc=1, device_id={"seq": other, "head": head}, device_id_type=MESH)

    greet(xp)
    greet(xm)

    @pl.when(jnp.logical_not(last_row))
    def _():
        greet(zp)

    @pl.when(jnp.logical_not(first_row))
    def _():
        greet(zm)

    for peer in peers:
        pl.semaphore_signal(barrier, inc=1, device_id={"seq": seq, "head": peer}, device_id_type=MESH)

    for here in range(XS):
        @pl.when(x == here)
        def _():
            for table, values in zip((ops, bounds, rows), PLAN[here]):
                for i, value in enumerate(values):
                    table[i] = value

    load_k.wait()
    load_v.wait()
    ends = jnp.where(jnp.logical_or(first_row, last_row), 1, 0)
    pl.semaphore_wait(barrier, 4 + KV_HEADS - 1 - ends)

    def operate(i, carry):
        value = ops[i]
        kind = lax.div(value, 16384)
        row = lax.rem(lax.div(value, 4096), 4)
        src = lax.rem(lax.div(value, 64), 64)
        dst = lax.rem(value, 64)
        here = z >= row

        @pl.when(jnp.logical_and(kind == 3, here))
        def _():
            pltpu.make_async_copy(kv.at[src], kv.at[src], recv_sems.at[src]).wait()

        wanted = jnp.logical_or(kind < 2, jnp.logical_and(kind == 2, z < ZS - 1))

        @pl.when(jnp.logical_and(wanted, here))
        def _():
            there = jnp.where(kind == 0, xp, jnp.where(kind == 1, xm, zp))
            pltpu.make_async_remote_copy(
                src_ref=kv.at[src],
                dst_ref=kv.at[dst],
                send_sem=send_sems.at[kind, row],
                recv_sem=recv_sems.at[dst],
                device_id={"seq": there, "head": head},
                device_id_type=MESH,
            ).start()

        return carry

    lax.fori_loop(0, bounds[0], operate, 0)
    pair = jnp.int32(PLAN[0][4])
    for here in range(1, XS):
        pair = jnp.where(x == here, PLAN[here][4], pair)

    for c in range(4):
        part = kv[OWN + c, 1].T.astype(jnp.float32)
        stat[0:1, pl.ds(c * CHUNK, CHUNK)] = jnp.max(part, axis=0, keepdims=True)
        stat[1:2, pl.ds(c * CHUNK, CHUNK)] = jnp.min(part, axis=0, keepdims=True)
        keys = kv[OWN + c, 0].astype(jnp.float32)
        low = jnp.min(keys, axis=0, keepdims=True)
        key_low[pl.ds(c, 1), :] = low
        key_step[pl.ds(c, 1), :] = (jnp.max(keys, axis=0, keepdims=True) - low) / 3.0

    load_q.wait()
    for t in range(TILES):
        p, h = divmod(t, PER)
        part = qv[pl.ds(p * TILE, TILE), pl.ds(h * HEAD_DIM, HEAD_DIM)].T.astype(jnp.float32) * SCALE
        high = part.astype(jnp.bfloat16)
        qt[t, 0:HEAD_DIM, :] = high
        qt[t, HEAD_DIM:, :] = (part - high.astype(jnp.float32)).astype(jnp.bfloat16)
        top[t] = jnp.full((1, TILE), NEG, jnp.float32)
        acc[t] = jnp.zeros((DEEP, TILE), jnp.float32)

    def score(keys, t, mode):
        s = jnp.dot(keys, qt[t], preferred_element_type=jnp.float32)
        if mode != "all":
            row = lax.broadcasted_iota(jnp.int32, s.shape, 0)
            col = lax.broadcasted_iota(jnp.int32, s.shape, 1)
            s = jnp.where(row <= col if mode == "past" else row > col, s, NEG)
        scores[t] = s

    def weigh(t):
        s = scores[t]
        old = top[t]
        new = jnp.maximum(old, jnp.max(s, axis=0, keepdims=True))
        weights[t] = jnp.exp2(s - new).astype(jnp.bfloat16)
        factor[t] = jnp.exp2(old - new)
        top[t] = new

    def gather(values, t):
        acc[t] = acc[t] * factor[t] + jnp.dot(values, weights[t], preferred_element_type=jnp.float32)

    def attend(first, second, modes, before=FULL_OUT):
        past = held[...]
        keys = jnp.concatenate([kv[first, 0], kv[second, 0]], axis=0)
        keys = jnp.concatenate([keys, keys], axis=1)
        values = jnp.concatenate([kv[first, 1].T, kv[second, 1].T], axis=1)
        values = jnp.concatenate([values, jnp.ones((DEEP - HEAD_DIM, 2 * CHUNK), jnp.bfloat16)], axis=0)
        jobs = tuple(t for t in range(TILES) if modes[t // PER] is not None)
        to_weigh = before[0] + jobs
        to_gather = before[1] + jobs
        for i, t in enumerate(jobs):
            score(keys, t, modes[t // PER])
            if to_weigh[i] is not None:
                weigh(to_weigh[i])
            if to_gather[i] is not None:
                gather(past if i < 4 else values, to_gather[i])
        held[...] = values

    attend(OWN, OWN + 1, ("past", "all"), before=((None,) * 2, (None,) * 4))

    for d, peer in enumerate(peers):
        pltpu.make_async_remote_copy(
            src_ref=stat,
            dst_ref=gathered.at[head],
            send_sem=stat_send.at[d],
            recv_sem=stat_recv.at[head],
            device_id={"seq": seq, "head": peer},
            device_id_type=MESH,
        ).start()

    attend(OWN + 2, OWN + 3, (None, "past"))

    def step(e, carry):
        lax.fori_loop(bounds[e], bounds[e + 1], operate, 0)
        slot = 2 * e + jnp.where(e > pair, 2, 0)
        there = z >= rows[e]

        @pl.when(jnp.logical_and(there, e != pair))
        def _():
            attend(slot, slot + 1, ("all", "all"))

        @pl.when(jnp.logical_and(there, e == pair))
        def _():
            attend(slot, slot + 1, ("after", None))
            attend(slot + 2, slot + 3, ("all", "after"), before=TAIL_OUT)

        return carry

    lax.fori_loop(0, STEPS - 1, step, 0)

    most, least = stat[0:1, :], stat[1:2, :]
    for peer in peers:
        pltpu.make_async_copy(gathered.at[peer], gathered.at[peer], stat_recv.at[peer]).wait()
        most = jnp.maximum(most, gathered[peer, 0:1, :])
        least = jnp.minimum(least, gathered[peer, 1:2, :])
    value_low[...] = least
    value_step[...] = (most - least) / 3.0
    for d in range(KV_HEADS - 1):
        pltpu.make_async_copy(stat, stat, stat_send.at[d]).wait()

    lax.fori_loop(STEPS - 1, STEPS, step, 0)
    past = held[...]
    for t in FULL_OUT[0]:
        weigh(t)
    for t in FULL_OUT[1]:
        gather(past, t)

    for here in range(XS):
        @pl.when(x == here)
        def _():
            for d in range(3):
                for row in range(REACH):
                    count = PLAN[here][3][d][row]
                    if count:
                        @pl.when(jnp.logical_and(z >= row, z < ZS - 1) if d == 2 else z >= row)
                        def _():
                            block = kv.at[pl.ds(0, count)]
                            pltpu.make_async_copy(block, block, send_sems.at[d, row]).wait()


def finish(acc, key_low, key_step, value_low, value_step, out_hbm, *rest):
    small, (out_v, sems) = rest[:4], rest[4:]
    copies = [
        pltpu.make_async_copy(src, dst, sems.at[i])
        for i, (src, dst) in enumerate(zip((key_low, key_step, value_low, value_step), small))
    ]
    for copy in copies:
        copy.start()
    for t in range(TILES):
        p, h = divmod(t, PER)
        part = acc[t, 0:HEAD_DIM] * (1.0 / acc[t, HEAD_DIM : HEAD_DIM + 1])
        out_v[pl.ds(p * TILE, TILE), pl.ds(h * HEAD_DIM, HEAD_DIM)] = part.astype(jnp.bfloat16).T
        if h == PER - 1:
            block = pl.ds(p * TILE, TILE)
            copies.append(pltpu.make_async_copy(out_v.at[block], out_hbm.at[block], sems.at[4 + p]))
            copies[-1].start()
    for copy in copies:
        copy.wait()


def shards(queries, new_keys, new_values):
    hbm = pl.BlockSpec(memory_space=pl.ANY)
    vmem = pl.BlockSpec(memory_space=pltpu.VMEM)
    f32, bf16 = jnp.float32, jnp.bfloat16
    chunks = TOK // CHUNK
    small = (
        ((chunks, HEAD_DIM), f32),
        ((chunks, HEAD_DIM), f32),
        ((1, TOK), f32),
        ((1, TOK), f32),
    )
    state = pl.pallas_call(
        kernel,
        out_shape=(pltpu.VMEM((TILES, DEEP, TILE), f32),) + tuple(pltpu.VMEM(*one) for one in small),
        in_specs=[hbm] * 3,
        out_specs=(vmem,) * 5,
        scratch_shapes=[
            pltpu.VMEM((OWN + 4, 2, CHUNK, HEAD_DIM), bf16),
            pltpu.VMEM((TOK, PER * HEAD_DIM), bf16),
            pltpu.VMEM((TILES, 2 * HEAD_DIM, TILE), bf16),
            pltpu.VMEM((TILES, 2 * CHUNK, TILE), f32),
            pltpu.VMEM((TILES, 2 * CHUNK, TILE), bf16),
            pltpu.VMEM((TILES, 1, TILE), f32),
            pltpu.VMEM((TILES, 1, TILE), f32),
            pltpu.VMEM((DEEP, 2 * CHUNK), bf16),
            pltpu.VMEM((2, TOK), f32),
            pltpu.VMEM((KV_HEADS, 2, TOK), f32),
            pltpu.SMEM((OPS,), jnp.int32),
            pltpu.SMEM((STEPS + 1,), jnp.int32),
            pltpu.SMEM((STEPS,), jnp.int32),
            pltpu.SemaphoreType.DMA((3,)),
            pltpu.SemaphoreType.DMA((OWN,)),
            pltpu.SemaphoreType.DMA((3, REACH)),
            pltpu.SemaphoreType.DMA((KV_HEADS - 1,)),
            pltpu.SemaphoreType.DMA((KV_HEADS,)),
        ],
        compiler_params=pltpu.CompilerParams(collective_id=0, has_side_effects=True),
    )(
        queries,
        new_keys.reshape(chunks, CHUNK, HEAD_DIM),
        new_values.reshape(chunks, CHUNK, HEAD_DIM),
    )
    state = [pltpu.with_memory_space_constraint(part, pltpu.VMEM) for part in state]
    attended, key_low, key_step, value_low, value_step = pl.pallas_call(
        finish,
        out_shape=(jax.ShapeDtypeStruct((TOK, PER * HEAD_DIM), bf16),)
        + tuple(jax.ShapeDtypeStruct(*one) for one in small),
        in_specs=[vmem] * 5,
        out_specs=(hbm,) * 5,
        scratch_shapes=[
            pltpu.VMEM((TOK, PER * HEAD_DIM), bf16),
            pltpu.SemaphoreType.DMA((4 + TOK // TILE,)),
        ],
    )(*state)
    return attended, key_low, key_step, value_low.reshape(TOK), value_step.reshape(TOK)


def solution(mesh):
    return jax.shard_map(
        shards,
        mesh=mesh,
        in_specs=(P("seq", "head"), P("seq", "head"), P("seq", "head")),
        out_specs=(P("seq", "head"), P("seq", "head"), P("seq", "head"), P("seq"), P("seq")),
        check_vma=False,
    )
```

```python
import math

import jax
import jax.numpy as jnp
from jax import lax
from jax.experimental import pallas as pl
from jax.experimental.pallas import tpu as pltpu
from jax.sharding import PartitionSpec as P

HEADS = 32
KV_HEADS = 8
HEAD_DIM = 128
WINDOW = 4096
GROUP = 128
PER = HEADS // KV_HEADS
TOK = 512
CHUNK = 128
TILE = 256
TILES = TOK // TILE * PER
DEEP = HEAD_DIM + 16
XS = 4
ZS = 8
REACH = 3
OWN = 32
STEPS = 15
SCALE = 1.4426950408889634 / math.sqrt(HEAD_DIM)
NEG = -1e30
MESH = pl.DeviceIdType.MESH

PLAN = (
    (
        (18434, 18499, 34881, 34950, 2123, 2180, 34816, 53312, 4167, 20557, 36945, 53632, 2245, 18574, 37266, 53248, 35015, 4102, 20492, 36880, 53440, 18639, 20695, 58432, 2058, 53504, 4366, 53376, 20630, 37006, 58496, 53568, 4431, 53952, 53696, 37331, 53760, 54080, 21339, 58368, 53824, 4693, 37469, 53888, 21150, 37526, 58240, 9112, 54016, 37658, 58304, 58560, 58624, 9500, 54848, 38495, 59200, 58688, 58816, 58752, 54784, 59072, 59008, 59136, 59264, 59328),
        (7, 20, 30, 33, 36, 43, 46, 50, 51, 54, 58, 60, 61, 63, 64, 66),
        (1, 1, 1, 1, 1, 1, 1, 2, 2, 2, 2, 1, 2, 2, 2),
        ((4, 5, 2), (4, 6, 0), (4, 9, 0)),
        8,
    ),
    (
        (2176, 35009, 34944, 34883, 34818, 2241, 49856, 53312, 2121, 4167, 20547, 36953, 49408, 33040, 53248, 4102, 20482, 53440, 2056, 4309, 20683, 37079, 53696, 54080, 21325, 53376, 20618, 37014, 49472, 337, 33105, 58944, 26191, 53760, 53632, 4498, 54272, 53824, 21081, 37459, 49792, 662, 58816, 26071, 54016, 54144, 58752, 59072, 26331, 54208, 5085, 37853, 54336, 5215, 58496, 25758, 54592, 38239, 58560, 54528, 58880, 59008, 59200, 59136, 59264, 59328),
        (6, 17, 28, 31, 36, 40, 42, 45, 52, 56, 59, 60, 61, 63, 65, 66),
        (1, 1, 0, 1, 1, 0, 1, 1, 1, 2, 1, 2, 2, 2, 2),
        ((6, 6, 0), (0, 6, 4), (6, 6, 0)),
        11,
    ),
    (
        (2180, 2123, 35013, 34818, 34883, 2245, 49152, 34948, 8, 53568, 20813, 37199, 49216, 73, 53376, 2058, 4240, 20616, 37004, 53440, 4305, 20681, 37069, 49728, 601, 55040, 53504, 20748, 37134, 53696, 58304, 25563, 50624, 53632, 58112, 25362, 53888, 21140, 37528, 49664, 536, 33300, 58176, 53952, 37593, 54592, 5471, 58240, 25498, 54464, 50240, 58880, 26142, 50176, 33822, 54400, 54528, 59008, 50560, 58944, 59072, 55104, 55168, 55232),
        (6, 14, 23, 29, 34, 42, 45, 49, 55, 56, 57, 59, 60, 61, 63, 64),
        (0, 1, 1, 1, 0, 1, 2, 0, 1, 1, 0, 2, 2, 1, 1),
        ((8, 3, 0), (0, 5, 4), (6, 6, 0)),
        6,
    ),
    (
        (34944, 35009, 34822, 49408, 34887, 33050, 53248, 4100, 20508, 36884, 49280, 49856, 53312, 4165, 36949, 49344, 16599, 49472, 53632, 4488, 20874, 37266, 49664, 53696, 4553, 20939, 37331, 54080, 21331, 54912, 5772, 49728, 50048, 17296, 33692, 58624, 9492, 25882, 49792, 54016, 58688, 9557, 25947, 54272, 5144, 50112, 33757, 54336, 58496, 9372, 54720, 50752, 58560, 54656, 55040, 50688, 54976, 55104, 55232, 55168),
        (3, 15, 17, 22, 27, 32, 39, 40, 47, 48, 53, 54, 57, 57, 60, 60),
        (1, 0, 0, 1, 0, 0, 1, 0, 1, 2, 1, 0, 1, 1, 1),
        ((0, 6, 3), (2, 4, 2), (7, 4, 0)),
        9,
    ),
)
OPS = max(len(plan[0]) for plan in PLAN)
TAIL_OUT = ((2, 3), (0, 1, 2, 3))
FULL_OUT = ((6, 7), (4, 5, 6, 7))


def kernel(
    q_hbm, k_hbm, v_hbm,
    acc, key_low, key_step, value_low, value_step,
    kv, qv, qt, scores, weights, factor, top, held, stat, gathered, ops, bounds, rows,
    local_sems, recv_sems, send_sems, stat_send, stat_recv,
):
    seq = lax.axis_index("seq")
    head = lax.axis_index("head")
    x = lax.rem(seq, XS)
    z = lax.div(seq, XS)
    xp = z * XS + lax.rem(x + 1, XS)
    xm = z * XS + lax.rem(x + XS - 1, XS)
    first_row, last_row = z == 0, z == ZS - 1
    zp = jnp.where(last_row, seq, seq + XS)
    zm = jnp.where(first_row, seq, seq - XS)
    peers = [lax.rem(head + d, KV_HEADS) for d in range(1, KV_HEADS)]

    load_k = pltpu.make_async_copy(k_hbm, kv.at[pl.ds(OWN, 4), 0], local_sems.at[0])
    load_v = pltpu.make_async_copy(v_hbm, kv.at[pl.ds(OWN, 4), 1], local_sems.at[1])
    load_q = pltpu.make_async_copy(q_hbm, qv, local_sems.at[2])
    load_k.start()
    load_v.start()
    load_q.start()

    barrier = pltpu.get_barrier_semaphore()

    def greet(other):
        pl.semaphore_signal(barrier, inc=1, device_id={"seq": other, "head": head}, device_id_type=MESH)

    greet(xp)
    greet(xm)

    @pl.when(jnp.logical_not(last_row))
    def _():
        greet(zp)

    @pl.when(jnp.logical_not(first_row))
    def _():
        greet(zm)

    for peer in peers:
        pl.semaphore_signal(barrier, inc=1, device_id={"seq": seq, "head": peer}, device_id_type=MESH)

    for here in range(XS):
        @pl.when(x == here)
        def _():
            for table, values in zip((ops, bounds, rows), PLAN[here]):
                for i, value in enumerate(values):
                    table[i] = value

    load_k.wait()
    load_v.wait()
    ends = jnp.where(jnp.logical_or(first_row, last_row), 1, 0)
    pl.semaphore_wait(barrier, 4 + KV_HEADS - 1 - ends)

    def operate(i, carry):
        value = ops[i]
        kind = lax.div(value, 16384)
        row = lax.rem(lax.div(value, 4096), 4)
        src = lax.rem(lax.div(value, 64), 64)
        dst = lax.rem(value, 64)
        here = z >= row

        @pl.when(jnp.logical_and(kind == 3, here))
        def _():
            pltpu.make_async_copy(kv.at[src], kv.at[src], recv_sems.at[src]).wait()

        wanted = jnp.logical_or(kind < 2, jnp.logical_and(kind == 2, z < ZS - 1))

        @pl.when(jnp.logical_and(wanted, here))
        def _():
            there = jnp.where(kind == 0, xp, jnp.where(kind == 1, xm, zp))
            pltpu.make_async_remote_copy(
                src_ref=kv.at[src],
                dst_ref=kv.at[dst],
                send_sem=send_sems.at[kind, row],
                recv_sem=recv_sems.at[dst],
                device_id={"seq": there, "head": head},
                device_id_type=MESH,
            ).start()

        return carry

    lax.fori_loop(0, bounds[0], operate, 0)
    pair = jnp.int32(PLAN[0][4])
    for here in range(1, XS):
        pair = jnp.where(x == here, PLAN[here][4], pair)

    for c in range(4):
        part = kv[OWN + c, 1].T.astype(jnp.float32)
        stat[0:1, pl.ds(c * CHUNK, CHUNK)] = jnp.max(part, axis=0, keepdims=True)
        stat[1:2, pl.ds(c * CHUNK, CHUNK)] = jnp.min(part, axis=0, keepdims=True)
        keys = kv[OWN + c, 0].astype(jnp.float32)
        low = jnp.min(keys, axis=0, keepdims=True)
        key_low[pl.ds(c, 1), :] = low
        key_step[pl.ds(c, 1), :] = (jnp.max(keys, axis=0, keepdims=True) - low) / 3.0

    load_q.wait()
    for t in range(TILES):
        p, h = divmod(t, PER)
        part = qv[pl.ds(p * TILE, TILE), pl.ds(h * HEAD_DIM, HEAD_DIM)].T.astype(jnp.float32) * SCALE
        high = part.astype(jnp.bfloat16)
        qt[t, 0:HEAD_DIM, :] = high
        qt[t, HEAD_DIM:, :] = (part - high.astype(jnp.float32)).astype(jnp.bfloat16)
        top[t] = jnp.full((1, TILE), NEG, jnp.float32)
        acc[t] = jnp.zeros((DEEP, TILE), jnp.float32)

    def score(keys, t, mode):
        s = jnp.dot(keys, qt[t], preferred_element_type=jnp.float32)
        if mode != "all":
            row = lax.broadcasted_iota(jnp.int32, s.shape, 0)
            col = lax.broadcasted_iota(jnp.int32, s.shape, 1)
            s = jnp.where(row <= col if mode == "past" else row > col, s, NEG)
        scores[t] = s

    def weigh(t):
        s = scores[t]
        old = top[t]
        new = jnp.maximum(old, jnp.max(s, axis=0, keepdims=True))
        weights[t] = jnp.exp2(s - new).astype(jnp.bfloat16)
        factor[t] = jnp.exp2(old - new)
        top[t] = new

    def gather(values, t):
        acc[t] = acc[t] * factor[t] + jnp.dot(values, weights[t], preferred_element_type=jnp.float32)

    def attend(first, second, modes, before=FULL_OUT):
        past = held[...]
        keys = jnp.concatenate([kv[first, 0], kv[second, 0]], axis=0)
        keys = jnp.concatenate([keys, keys], axis=1)
        values = jnp.concatenate([kv[first, 1].T, kv[second, 1].T], axis=1)
        values = jnp.concatenate([values, jnp.ones((DEEP - HEAD_DIM, 2 * CHUNK), jnp.bfloat16)], axis=0)
        jobs = tuple(t for t in range(TILES) if modes[t // PER] is not None)
        to_weigh = before[0] + jobs
        to_gather = before[1] + jobs
        for i, t in enumerate(jobs):
            score(keys, t, modes[t // PER])
            if to_weigh[i] is not None:
                weigh(to_weigh[i])
            if to_gather[i] is not None:
                gather(past if i < 4 else values, to_gather[i])
        held[...] = values

    attend(OWN, OWN + 1, ("past", "all"), before=((None,) * 2, (None,) * 4))

    for d, peer in enumerate(peers):
        pltpu.make_async_remote_copy(
            src_ref=stat,
            dst_ref=gathered.at[head],
            send_sem=stat_send.at[d],
            recv_sem=stat_recv.at[head],
            device_id={"seq": seq, "head": peer},
            device_id_type=MESH,
        ).start()

    attend(OWN + 2, OWN + 3, (None, "past"))

    def step(e, carry):
        lax.fori_loop(bounds[e], bounds[e + 1], operate, 0)
        slot = 2 * e + jnp.where(e > pair, 2, 0)
        there = z >= rows[e]

        @pl.when(jnp.logical_and(there, e != pair))
        def _():
            attend(slot, slot + 1, ("all", "all"))

        @pl.when(jnp.logical_and(there, e == pair))
        def _():
            attend(slot, slot + 1, ("after", None))
            attend(slot + 2, slot + 3, ("all", "after"), before=TAIL_OUT)

        return carry

    lax.fori_loop(0, STEPS - 1, step, 0)

    most, least = stat[0:1, :], stat[1:2, :]
    for peer in peers:
        pltpu.make_async_copy(gathered.at[peer], gathered.at[peer], stat_recv.at[peer]).wait()
        most = jnp.maximum(most, gathered[peer, 0:1, :])
        least = jnp.minimum(least, gathered[peer, 1:2, :])
    value_low[...] = least
    value_step[...] = (most - least) / 3.0
    for d in range(KV_HEADS - 1):
        pltpu.make_async_copy(stat, stat, stat_send.at[d]).wait()

    lax.fori_loop(STEPS - 1, STEPS, step, 0)
    past = held[...]
    for t in FULL_OUT[0]:
        weigh(t)
    for t in FULL_OUT[1]:
        gather(past, t)

    for here in range(XS):
        @pl.when(x == here)
        def _():
            for d in range(3):
                for row in range(REACH):
                    count = PLAN[here][3][d][row]
                    if count:
                        @pl.when(jnp.logical_and(z >= row, z < ZS - 1) if d == 2 else z >= row)
                        def _():
                            block = kv.at[pl.ds(0, count)]
                            pltpu.make_async_copy(block, block, send_sems.at[d, row]).wait()


def finish(acc, key_low, key_step, value_low, value_step, out_hbm, *rest):
    small, (out_v, sems) = rest[:4], rest[4:]
    copies = [
        pltpu.make_async_copy(src, dst, sems.at[i])
        for i, (src, dst) in enumerate(zip((key_low, key_step, value_low, value_step), small))
    ]
    for copy in copies:
        copy.start()
    for t in range(TILES):
        p, h = divmod(t, PER)
        part = acc[t, 0:HEAD_DIM] * (1.0 / acc[t, HEAD_DIM : HEAD_DIM + 1])
        out_v[pl.ds(p * TILE, TILE), pl.ds(h * HEAD_DIM, HEAD_DIM)] = part.astype(jnp.bfloat16).T
        if h == PER - 1:
            block = pl.ds(p * TILE, TILE)
            copies.append(pltpu.make_async_copy(out_v.at[block], out_hbm.at[block], sems.at[4 + p]))
            copies[-1].start()
    for copy in copies:
        copy.wait()


def shards(queries, new_keys, new_values):
    hbm = pl.BlockSpec(memory_space=pl.ANY)
    vmem = pl.BlockSpec(memory_space=pltpu.VMEM)
    f32, bf16 = jnp.float32, jnp.bfloat16
    chunks = TOK // CHUNK
    small = (
        ((chunks, HEAD_DIM), f32),
        ((chunks, HEAD_DIM), f32),
        ((1, TOK), f32),
        ((1, TOK), f32),
    )
    state = pl.pallas_call(
        kernel,
        out_shape=(pltpu.VMEM((TILES, DEEP, TILE), f32),) + tuple(pltpu.VMEM(*one) for one in small),
        in_specs=[hbm] * 3,
        out_specs=(vmem,) * 5,
        scratch_shapes=[
            pltpu.VMEM((OWN + 4, 2, CHUNK, HEAD_DIM), bf16),
            pltpu.VMEM((TOK, PER * HEAD_DIM), bf16),
            pltpu.VMEM((TILES, 2 * HEAD_DIM, TILE), bf16),
            pltpu.VMEM((TILES, 2 * CHUNK, TILE), f32),
            pltpu.VMEM((TILES, 2 * CHUNK, TILE), bf16),
            pltpu.VMEM((TILES, 1, TILE), f32),
            pltpu.VMEM((TILES, 1, TILE), f32),
            pltpu.VMEM((DEEP, 2 * CHUNK), bf16),
            pltpu.VMEM((2, TOK), f32),
            pltpu.VMEM((KV_HEADS, 2, TOK), f32),
            pltpu.SMEM((OPS,), jnp.int32),
            pltpu.SMEM((STEPS + 1,), jnp.int32),
            pltpu.SMEM((STEPS,), jnp.int32),
            pltpu.SemaphoreType.DMA((3,)),
            pltpu.SemaphoreType.DMA((OWN,)),
            pltpu.SemaphoreType.DMA((3, REACH)),
            pltpu.SemaphoreType.DMA((KV_HEADS - 1,)),
            pltpu.SemaphoreType.DMA((KV_HEADS,)),
        ],
        compiler_params=pltpu.CompilerParams(collective_id=0, has_side_effects=True),
    )(
        queries,
        new_keys.reshape(chunks, CHUNK, HEAD_DIM),
        new_values.reshape(chunks, CHUNK, HEAD_DIM),
    )
    state = [pltpu.with_memory_space_constraint(part, pltpu.VMEM) for part in state]
    attended, key_low, key_step, value_low, value_step = pl.pallas_call(
        finish,
        out_shape=(jax.ShapeDtypeStruct((TOK, PER * HEAD_DIM), bf16),)
        + tuple(jax.ShapeDtypeStruct(*one) for one in small),
        in_specs=[vmem] * 5,
        out_specs=(hbm,) * 5,
        scratch_shapes=[
            pltpu.VMEM((TOK, PER * HEAD_DIM), bf16),
            pltpu.SemaphoreType.DMA((4 + TOK // TILE,)),
        ],
    )(*state)
    return attended, key_low, key_step, value_low.reshape(TOK), value_step.reshape(TOK)


def solution(mesh):
    return jax.shard_map(
        shards,
        mesh=mesh,
        in_specs=(P("seq", "head"), P("seq", "head"), P("seq", "head")),
        out_specs=(P("seq", "head"), P("seq", "head"), P("seq", "head"), P("seq"), P("seq")),
        check_vma=False,
    )
```

```python
import math

import jax
import jax.numpy as jnp
from jax import lax
from jax.experimental import pallas as pl
from jax.experimental.pallas import tpu as pltpu
from jax.sharding import PartitionSpec as P

HEADS = 32
KV_HEADS = 8
HEAD_DIM = 128
WINDOW = 4096
GROUP = 128
PER = HEADS // KV_HEADS
TOK = 512
CHUNK = 128
TILE = 256
TILES = TOK // TILE * PER
DEEP = HEAD_DIM + 16
XS = 4
ZS = 8
REACH = 3
OWN = 32
STEPS = 15
SCALE = 1.4426950408889634 / math.sqrt(HEAD_DIM)
NEG = -1e30
MESH = pl.DeviceIdType.MESH

PLAN = (
    (
        (2052, 34881, 34816, 18633, 18434, 18499, 34946, 53312, 35011, 4169, 20557, 36941, 53248, 18568, 2117, 20492, 36876, 53376, 2188, 20628, 37006, 53504, 20760, 53440, 20693, 37071, 53632, 4494, 53568, 20825, 37203, 58176, 53696, 4559, 37333, 53760, 58112, 53952, 4819, 53824, 21087, 37465, 58240, 53888, 4754, 58304, 54336, 37979, 54272, 58560, 9433, 58496, 58624, 58688, 9565, 54720, 38367, 54656, 58944, 58880, 59200, 59072, 59008, 59136, 59328, 59264),
        (7, 17, 26, 31, 35, 42, 45, 48, 51, 53, 57, 58, 60, 63, 64, 66),
        (1, 1, 1, 1, 1, 1, 2, 1, 2, 2, 1, 2, 2, 2, 2),
        ((3, 5, 2), (4, 7, 0), (4, 9, 0)),
        6,
    ),
    (
        (34816, 34881, 34946, 2184, 49408, 2117, 35011, 278, 33032, 53248, 20484, 36888, 53312, 2052, 2249, 4181, 20549, 53376, 4242, 20616, 37018, 53824, 53632, 37264, 53440, 4307, 20681, 37083, 49472, 343, 53696, 20945, 53760, 49920, 794, 33556, 53888, 58880, 26130, 53952, 21207, 59008, 26264, 54144, 49984, 33621, 58368, 25626, 54208, 59072, 58432, 54464, 38111, 54528, 5406, 58752, 26014, 54400, 38046, 54592, 58816, 58944, 59328, 59136, 59200, 59264),
        (4, 17, 28, 30, 33, 39, 41, 46, 49, 51, 59, 60, 61, 62, 65, 66),
        (1, 1, 0, 1, 1, 1, 0, 1, 2, 1, 1, 2, 2, 2, 2),
        ((7, 4, 0), (0, 6, 4), (7, 6, 0)),
        12,
    ),
    (
        (34944, 2182, 35009, 34818, 2062, 49664, 540, 53248, 34883, 2247, 20486, 36878, 53312, 4171, 20551, 36943, 53376, 4250, 20618, 37004, 49472, 2127, 343, 53632, 53440, 20683, 37069, 50560, 34192, 50880, 18125, 58240, 49408, 278, 33044, 53696, 58304, 25553, 49728, 605, 53952, 58112, 25366, 54592, 53888, 37532, 58176, 25431, 54400, 5278, 54336, 54272, 54464, 58880, 26140, 54528, 50624, 58944, 59136, 50816, 59200, 55168, 55232),
        (5, 16, 27, 35, 38, 43, 46, 48, 52, 55, 56, 59, 59, 61, 62, 63),
        (1, 1, 0, 1, 0, 1, 2, 1, 1, 1, 0, 2, 0, 2, 1),
        ((8, 3, 0), (1, 4, 4), (6, 5, 0)),
        6,
    ),
    (
        (34816, 34881, 35013, 49536, 34948, 33162, 53248, 4102, 20486, 36880, 49728, 16987, 50048, 53312, 4167, 20551, 36945, 49280, 53568, 4427, 20811, 37203, 49344, 50944, 53504, 4362, 20746, 37138, 54080, 21329, 49600, 53888, 4752, 49664, 53952, 58368, 9236, 25624, 54016, 54912, 5782, 58432, 25689, 54528, 50112, 33755, 58560, 9437, 25821, 54784, 50624, 58496, 9372, 54592, 21855, 50560, 54848, 54976, 51008, 55232, 55168),
        (3, 17, 23, 28, 31, 34, 35, 39, 46, 53, 56, 57, 59, 60, 61, 61),
        (1, 0, 1, 0, 0, 1, 1, 0, 2, 1, 0, 1, 1, 0, 1),
        ((0, 6, 3), (1, 6, 3), (6, 4, 0)),
        8,
    ),
)
OPS = max(len(plan[0]) for plan in PLAN)
TAIL_OUT = ((2, 3), (0, 1, 2, 3))
FULL_OUT = ((6, 7), (4, 5, 6, 7))


def kernel(
    q_hbm, k_hbm, v_hbm,
    acc, key_low, key_step, value_low, value_step,
    kv, qv, qt, scores, weights, factor, top, held, stat, gathered, ops, bounds, rows,
    local_sems, recv_sems, send_sems, stat_send, stat_recv,
):
    seq = lax.axis_index("seq")
    head = lax.axis_index("head")
    x = lax.rem(seq, XS)
    z = lax.div(seq, XS)
    xp = z * XS + lax.rem(x + 1, XS)
    xm = z * XS + lax.rem(x + XS - 1, XS)
    first_row, last_row = z == 0, z == ZS - 1
    zp = jnp.where(last_row, seq, seq + XS)
    zm = jnp.where(first_row, seq, seq - XS)
    peers = [lax.rem(head + d, KV_HEADS) for d in range(1, KV_HEADS)]

    load_k = pltpu.make_async_copy(k_hbm, kv.at[pl.ds(OWN, 4), 0], local_sems.at[0])
    load_v = pltpu.make_async_copy(v_hbm, kv.at[pl.ds(OWN, 4), 1], local_sems.at[1])
    load_q = pltpu.make_async_copy(q_hbm, qv, local_sems.at[2])
    load_k.start()
    load_v.start()
    load_q.start()

    barrier = pltpu.get_barrier_semaphore()

    def greet(other):
        pl.semaphore_signal(barrier, inc=1, device_id={"seq": other, "head": head}, device_id_type=MESH)

    greet(xp)
    greet(xm)

    @pl.when(jnp.logical_not(last_row))
    def _():
        greet(zp)

    @pl.when(jnp.logical_not(first_row))
    def _():
        greet(zm)

    for peer in peers:
        pl.semaphore_signal(barrier, inc=1, device_id={"seq": seq, "head": peer}, device_id_type=MESH)

    for here in range(XS):
        @pl.when(x == here)
        def _():
            for table, values in zip((ops, bounds, rows), PLAN[here]):
                for i, value in enumerate(values):
                    table[i] = value

    load_k.wait()
    load_v.wait()
    ends = jnp.where(jnp.logical_or(first_row, last_row), 1, 0)
    pl.semaphore_wait(barrier, 4 + KV_HEADS - 1 - ends)

    def operate(i, carry):
        value = ops[i]
        kind = lax.div(value, 16384)
        row = lax.rem(lax.div(value, 4096), 4)
        src = lax.rem(lax.div(value, 64), 64)
        dst = lax.rem(value, 64)
        here = z >= row

        @pl.when(jnp.logical_and(kind == 3, here))
        def _():
            pltpu.make_async_copy(kv.at[src], kv.at[src], recv_sems.at[src]).wait()

        wanted = jnp.logical_or(kind < 2, jnp.logical_and(kind == 2, z < ZS - 1))

        @pl.when(jnp.logical_and(wanted, here))
        def _():
            there = jnp.where(kind == 0, xp, jnp.where(kind == 1, xm, zp))
            pltpu.make_async_remote_copy(
                src_ref=kv.at[src],
                dst_ref=kv.at[dst],
                send_sem=send_sems.at[kind, row],
                recv_sem=recv_sems.at[dst],
                device_id={"seq": there, "head": head},
                device_id_type=MESH,
            ).start()

        return carry

    lax.fori_loop(0, bounds[0], operate, 0)
    pair = jnp.int32(PLAN[0][4])
    for here in range(1, XS):
        pair = jnp.where(x == here, PLAN[here][4], pair)

    for c in range(4):
        part = kv[OWN + c, 1].T.astype(jnp.float32)
        stat[0:1, pl.ds(c * CHUNK, CHUNK)] = jnp.max(part, axis=0, keepdims=True)
        stat[1:2, pl.ds(c * CHUNK, CHUNK)] = jnp.min(part, axis=0, keepdims=True)
        keys = kv[OWN + c, 0].astype(jnp.float32)
        low = jnp.min(keys, axis=0, keepdims=True)
        key_low[pl.ds(c, 1), :] = low
        key_step[pl.ds(c, 1), :] = (jnp.max(keys, axis=0, keepdims=True) - low) / 3.0

    load_q.wait()
    for t in range(TILES):
        p, h = divmod(t, PER)
        part = qv[pl.ds(p * TILE, TILE), pl.ds(h * HEAD_DIM, HEAD_DIM)].T.astype(jnp.float32) * SCALE
        high = part.astype(jnp.bfloat16)
        qt[t, 0:HEAD_DIM, :] = high
        qt[t, HEAD_DIM:, :] = (part - high.astype(jnp.float32)).astype(jnp.bfloat16)
        top[t] = jnp.full((1, TILE), NEG, jnp.float32)
        acc[t] = jnp.zeros((DEEP, TILE), jnp.float32)

    def score(keys, t, mode):
        s = jnp.dot(keys, qt[t], preferred_element_type=jnp.float32)
        if mode != "all":
            row = lax.broadcasted_iota(jnp.int32, s.shape, 0)
            col = lax.broadcasted_iota(jnp.int32, s.shape, 1)
            s = jnp.where(row <= col if mode == "past" else row > col, s, NEG)
        scores[t] = s

    def weigh(t):
        s = scores[t]
        old = top[t]
        new = jnp.maximum(old, jnp.max(s, axis=0, keepdims=True))
        weights[t] = jnp.exp2(s - new).astype(jnp.bfloat16)
        factor[t] = jnp.exp2(old - new)
        top[t] = new

    def gather(values, t):
        acc[t] = acc[t] * factor[t] + jnp.dot(values, weights[t], preferred_element_type=jnp.float32)

    def attend(first, second, modes, before=FULL_OUT):
        past = held[...]
        keys = jnp.concatenate([kv[first, 0], kv[second, 0]], axis=0)
        keys = jnp.concatenate([keys, keys], axis=1)
        values = jnp.concatenate([kv[first, 1].T, kv[second, 1].T], axis=1)
        values = jnp.concatenate([values, jnp.ones((DEEP - HEAD_DIM, 2 * CHUNK), jnp.bfloat16)], axis=0)
        jobs = tuple(t for t in range(TILES) if modes[t // PER] is not None)
        to_weigh = before[0] + jobs
        to_gather = before[1] + jobs
        for i, t in enumerate(jobs):
            score(keys, t, modes[t // PER])
            if to_weigh[i] is not None:
                weigh(to_weigh[i])
            if to_gather[i] is not None:
                gather(past if i < 4 else values, to_gather[i])
        held[...] = values

    attend(OWN, OWN + 1, ("past", "all"), before=((None,) * 2, (None,) * 4))

    for d, peer in enumerate(peers):
        pltpu.make_async_remote_copy(
            src_ref=stat,
            dst_ref=gathered.at[head],
            send_sem=stat_send.at[d],
            recv_sem=stat_recv.at[head],
            device_id={"seq": seq, "head": peer},
            device_id_type=MESH,
        ).start()

    attend(OWN + 2, OWN + 3, (None, "past"))

    def step(e, carry):
        lax.fori_loop(bounds[e], bounds[e + 1], operate, 0)
        slot = 2 * e + jnp.where(e > pair, 2, 0)
        there = z >= rows[e]

        @pl.when(jnp.logical_and(there, e != pair))
        def _():
            attend(slot, slot + 1, ("all", "all"))

        @pl.when(jnp.logical_and(there, e == pair))
        def _():
            attend(slot, slot + 1, ("after", None))
            attend(slot + 2, slot + 3, ("all", "after"), before=TAIL_OUT)

        return carry

    lax.fori_loop(0, STEPS - 1, step, 0)

    most, least = stat[0:1, :], stat[1:2, :]
    for peer in peers:
        pltpu.make_async_copy(gathered.at[peer], gathered.at[peer], stat_recv.at[peer]).wait()
        most = jnp.maximum(most, gathered[peer, 0:1, :])
        least = jnp.minimum(least, gathered[peer, 1:2, :])
    value_low[...] = least
    value_step[...] = (most - least) / 3.0
    for d in range(KV_HEADS - 1):
        pltpu.make_async_copy(stat, stat, stat_send.at[d]).wait()

    lax.fori_loop(STEPS - 1, STEPS, step, 0)
    past = held[...]
    for t in FULL_OUT[0]:
        weigh(t)
    for t in FULL_OUT[1]:
        gather(past, t)

    for here in range(XS):
        @pl.when(x == here)
        def _():
            for d in range(3):
                for row in range(REACH):
                    count = PLAN[here][3][d][row]
                    if count:
                        @pl.when(jnp.logical_and(z >= row, z < ZS - 1) if d == 2 else z >= row)
                        def _():
                            block = kv.at[pl.ds(0, count)]
                            pltpu.make_async_copy(block, block, send_sems.at[d, row]).wait()


def finish(acc, key_low, key_step, value_low, value_step, out_hbm, *rest):
    small, (out_v, sems) = rest[:4], rest[4:]
    copies = [
        pltpu.make_async_copy(src, dst, sems.at[i])
        for i, (src, dst) in enumerate(zip((key_low, key_step, value_low, value_step), small))
    ]
    for copy in copies:
        copy.start()
    for t in range(TILES):
        p, h = divmod(t, PER)
        part = acc[t, 0:HEAD_DIM] * (1.0 / acc[t, HEAD_DIM : HEAD_DIM + 1])
        out_v[pl.ds(p * TILE, TILE), pl.ds(h * HEAD_DIM, HEAD_DIM)] = part.astype(jnp.bfloat16).T
        if h % 2 == 1:
            block = (pl.ds(p * TILE, TILE), pl.ds((h - 1) * HEAD_DIM, 2 * HEAD_DIM))
            copies.append(pltpu.make_async_copy(out_v.at[block], out_hbm.at[block], sems.at[4 + t // 2]))
            copies[-1].start()
    for copy in copies:
        copy.wait()


def shards(queries, new_keys, new_values):
    hbm = pl.BlockSpec(memory_space=pl.ANY)
    vmem = pl.BlockSpec(memory_space=pltpu.VMEM)
    f32, bf16 = jnp.float32, jnp.bfloat16
    chunks = TOK // CHUNK
    small = (
        ((chunks, HEAD_DIM), f32),
        ((chunks, HEAD_DIM), f32),
        ((1, TOK), f32),
        ((1, TOK), f32),
    )
    state = pl.pallas_call(
        kernel,
        out_shape=(pltpu.VMEM((TILES, DEEP, TILE), f32),) + tuple(pltpu.VMEM(*one) for one in small),
        in_specs=[hbm] * 3,
        out_specs=(vmem,) * 5,
        scratch_shapes=[
            pltpu.VMEM((OWN + 4, 2, CHUNK, HEAD_DIM), bf16),
            pltpu.VMEM((TOK, PER * HEAD_DIM), bf16),
            pltpu.VMEM((TILES, 2 * HEAD_DIM, TILE), bf16),
            pltpu.VMEM((TILES, 2 * CHUNK, TILE), f32),
            pltpu.VMEM((TILES, 2 * CHUNK, TILE), bf16),
            pltpu.VMEM((TILES, 1, TILE), f32),
            pltpu.VMEM((TILES, 1, TILE), f32),
            pltpu.VMEM((DEEP, 2 * CHUNK), bf16),
            pltpu.VMEM((2, TOK), f32),
            pltpu.VMEM((KV_HEADS, 2, TOK), f32),
            pltpu.SMEM((OPS,), jnp.int32),
            pltpu.SMEM((STEPS + 1,), jnp.int32),
            pltpu.SMEM((STEPS,), jnp.int32),
            pltpu.SemaphoreType.DMA((3,)),
            pltpu.SemaphoreType.DMA((OWN,)),
            pltpu.SemaphoreType.DMA((3, REACH)),
            pltpu.SemaphoreType.DMA((KV_HEADS - 1,)),
            pltpu.SemaphoreType.DMA((KV_HEADS,)),
        ],
        compiler_params=pltpu.CompilerParams(collective_id=0, has_side_effects=True),
    )(
        queries,
        new_keys.reshape(chunks, CHUNK, HEAD_DIM),
        new_values.reshape(chunks, CHUNK, HEAD_DIM),
    )
    state = [pltpu.with_memory_space_constraint(part, pltpu.VMEM) for part in state]
    attended, key_low, key_step, value_low, value_step = pl.pallas_call(
        finish,
        out_shape=(jax.ShapeDtypeStruct((TOK, PER * HEAD_DIM), bf16),)
        + tuple(jax.ShapeDtypeStruct(*one) for one in small),
        in_specs=[vmem] * 5,
        out_specs=(hbm,) * 5,
        scratch_shapes=[
            pltpu.VMEM((TOK, PER * HEAD_DIM), bf16),
            pltpu.SemaphoreType.DMA((4 + TILES // 2,)),
        ],
    )(*state)
    return attended, key_low, key_step, value_low.reshape(TOK), value_step.reshape(TOK)


def solution(mesh):
    return jax.shard_map(
        shards,
        mesh=mesh,
        in_specs=(P("seq", "head"), P("seq", "head"), P("seq", "head")),
        out_specs=(P("seq", "head"), P("seq", "head"), P("seq", "head"), P("seq"), P("seq")),
        check_vma=False,
    )
```
